16 devices in a mesh: data: 2 (over y, z), tp: 8 (over x, core).
Axes of the slice: x: 4, y: 2, z: 1, core: 2. Of those that a mesh axis runs over, the one named last changes fastest.
The devices are a block of a 4x4x8 slice.
Arguments:
- X: bfloat16 [4096, 4096], P(('data', 'tp')), parts along dimension 0
- gamma: float32 [4096], replicated
- W1: bfloat16 [4096, 14336], P(None, 'tp')
- W2: bfloat16 [14336, 4096], P('tp')
- dY: bfloat16 [4096, 4096], P(('data', 'tp')), parts along dimension 0
Outputs:
- output 1: bfloat16 [4096, 4096], P(('data', 'tp')), parts along dimension 0
- output 2: bfloat16 [4096, 4096], P(('data', 'tp')), parts along dimension 0
- output 3: float32 [8192, 14336], P('data', 'tp'), parts along dimension 0
- output 4: float32 [28672, 4096], P(('data', 'tp')), parts along dimension 0
- output 5: float32 [8192], P('data'), parts along dimension 0
There are 2 independent parts. The reference program is written for one: setup_inputs(seed, part) draws one part's arguments, and reference() takes and returns one part's arrays. A program takes and returns all parts, laid end to end along the dimension named above; an argument that names none is the same for every part.
All inputs are finite; a program needn't handle non-finite values.
Results may differ from the reference program's by a relative error of at most 0.001.
Values are sent between devices in bfloat16 or wider.
A program may use at most 768 MiB of HBM per device.

```python
import jax
import jax.numpy as jnp
from jax import lax

S = 2048
D = 4096
F = 14336
EPS = 1e-6


def setup_inputs(seed: int = 0, part: int = 0) -> dict:
    key = jax.random.key(seed)
    kg, k1, k2, kbase = jax.random.split(key, 4)
    kx, ky = jax.random.split(jax.random.fold_in(kbase, part))
    X = jax.random.normal(kx, (S, D), jnp.float32).astype(jnp.bfloat16)
    gamma = 1.0 + 0.2 * jax.random.normal(kg, (D,), jnp.float32)
    W1 = (jax.random.normal(k1, (D, F), jnp.float32) * D ** -0.5).astype(jnp.bfloat16)
    W2 = (jax.random.normal(k2, (F, D), jnp.float32) * (1.5 * F ** -0.5)).astype(jnp.bfloat16)
    dY = jax.random.normal(ky, (S, D), jnp.float32).astype(jnp.bfloat16)
    return {"X": X, "gamma": gamma, "W1": W1, "W2": W2, "dY": dY}


def _gelu(a):
    return jax.nn.gelu(a, approximate=True)


def reference(X, gamma, W1, W2, dY):
    x = X.astype(jnp.float32)
    mu = jnp.mean(x, axis=-1, keepdims=True)
    xc = x - mu
    var = jnp.mean(xc * xc, axis=-1, keepdims=True)
    rstd = lax.rsqrt(var + EPS)
    xhatv = xc * rstd
    Xn = (xhatv * gamma).astype(jnp.bfloat16)
    A = jnp.dot(Xn, W1, preferred_element_type=jnp.float32)
    H = _gelu(A).astype(jnp.bfloat16)
    Y = (x + jnp.dot(H, W2, preferred_element_type=jnp.float32)).astype(jnp.bfloat16)
    dW2 = jnp.dot(H.T, dY, preferred_element_type=jnp.float32)
    dH = jnp.dot(dY, W2.T, preferred_element_type=jnp.float32)
    dA = jax.vjp(_gelu, A)[1](dH)[0].astype(jnp.bfloat16)
    dW1 = jnp.dot(Xn.T, dA, preferred_element_type=jnp.float32)
    dXn = jnp.dot(dA, W1.T, preferred_element_type=jnp.float32)
    dgamma = jnp.sum(dXn * xhatv, axis=0)
    dxhat = dXn * gamma
    dx = rstd * (dxhat - jnp.mean(dxhat, axis=-1, keepdims=True) - xhatv * jnp.mean(dxhat * xhatv, axis=-1, keepdims=True))
    dX = (dY.astype(jnp.float32) + dx).astype(jnp.bfloat16)
    return (Y, dX, dW1, dW2, dgamma)
```

```python
import functools

import jax
import jax.numpy as jnp
from jax import lax
from jax.experimental import pallas as pl
from jax.experimental.pallas import tpu as pltpu
from jax.sharding import PartitionSpec as P

EPS = 1e-6
BF = jnp.bfloat16
F32 = jnp.float32


def _gelu(a):
    return jax.nn.gelu(a, approximate=True)


def _ln(x):
    mu = jnp.mean(x, axis=-1, keepdims=True)
    xc = x - mu
    var = jnp.mean(xc * xc, axis=-1, keepdims=True)
    rstd = lax.rsqrt(var + EPS)
    return xc * rstd, rstd


def _tn(a, b):
    return lax.dot_general(a, b, (((0,), (0,)), ((), ())), preferred_element_type=F32)


TILE = 256
NCH = 512


def _nt(a, b):
    return lax.dot_general(a, b, (((1,), (1,)), ((), ())), preferred_element_type=F32)


def _ln_kernel(x_ref, gamma_ref, top_ref, bot_ref):
    h = top_ref.shape[0]
    gamma = gamma_ref[...]
    for out, r in ((top_ref, 0), (bot_ref, h)):
        out[...] = (_ln(x_ref[r:r + h, :].astype(F32))[0] * gamma).astype(BF)


def _norm(x, gamma):
    h = x.shape[0] // 2
    half = jax.ShapeDtypeStruct((h, x.shape[1]), BF)
    return pl.pallas_call(
        _ln_kernel, out_shape=(half, half), name="norm",
        compiler_params=pltpu.CompilerParams(vmem_limit_bytes=48 << 20),
        cost_estimate=pl.CostEstimate(flops=20 * x.size, bytes_accessed=4 * x.size, transcendentals=0),
    )(x, gamma.reshape(1, -1))


def _pass_kernel(mode, nx, nh, na, has_acc, *refs):
    refs = list(refs)

    def take(k):
        out, refs[:k] = refs[:k], []
        return out

    fwd, bwd = mode != "bwd", mode != "fwd"
    xs = take(nx) if fwd else []
    gs = take(nx) if bwd else []
    w1, w2 = take(nh), take(nh)
    a_in = [take(na) for _ in range(nh)] if not fwd else []
    y_in = take(nx) if fwd and has_acc else None
    d_in = take(nx) if bwd and has_acc else None
    a_out = take(nh) if mode == "fwd" else []
    h_out = take(nh) if fwd else []
    y_out = take(nx) if fwd else []
    da_out = take(nh) if bwd else []
    d_out = take(nx) if bwd else []
    xv = take(1)[0] if fwd else None
    gv = take(1)[0] if bwd else None

    @pl.when(pl.program_id(0) == 0)
    def _():
        for parts, v in ((xs, xv), (gs, gv)):
            r = 0
            for p in parts:
                v[r:r + p.shape[0], :] = p[...]
                r += p.shape[0]
        for outs, ins in ((y_out, y_in), (d_out, d_in)):
            for j, o in enumerate(outs):
                o[...] = ins[j][...] if ins else jnp.zeros_like(o)

    if fwd:
        a = [jnp.dot(xv[...], w1[k][...], preferred_element_type=F32) for k in range(nh)]
        h = [_gelu(v).astype(BF) for v in a]
        for k in range(nh):
            h_out[k][...] = h[k]
            if a_out:
                a_out[k][...] = a[k]
    else:
        a = [jnp.concatenate([p[...] for p in v]) for v in a_in]
    if bwd:
        dh = [_nt(gv[...], w2[k][...]) for k in range(nh)]
        da = [jax.vjp(_gelu, a[k])[1](dh[k])[0].astype(BF) for k in range(nh)]
        for k in range(nh):
            da_out[k][...] = da[k]

    def add(outs, n, v):
        r = 0
        for o in outs:
            m = o.shape[0]
            o[:, n:n + NCH] += v[r:r + m]
            r += m

    for n in range(0, w2[0].shape[1], NCH):
        if fwd:
            add(y_out, n, sum(jnp.dot(h[k], w2[k][:, n:n + NCH], preferred_element_type=F32) for k in range(nh)))
        if bwd:
            add(d_out, n, sum(_nt(da[k], w1[k][n:n + NCH, :]) for k in range(nh)))


def _pass(mode, ws, xs=(), gs=(), a=(), y=(), d=()):
    fwd, bwd = mode != "bwd", mode != "fwd"
    sizes = [p.shape[0] for p in (xs if fwd else gs)]
    nx, nh = len(sizes), len(ws)
    dm, f = ws[0][0].shape
    rows = sum(sizes)
    both = fwd + bwd
    once = pl.Buffered(buffer_count=1)

    def whole(r):
        return pl.BlockSpec((r, dm), lambda i: (0, 0), pipeline_mode=once)

    def cols(r):
        return pl.BlockSpec((r, TILE), lambda i: (0, i))

    pieces = [whole(r) for r in sizes]
    has_acc = bool(y or d)
    args = list(xs) * fwd + list(gs) * bwd + [w[0] for w in ws] + [w[1] for w in ws] + [p for v in a for p in v] + list(y) + list(d)
    in_specs = pieces * both + [cols(dm)] * nh + [pl.BlockSpec((TILE, dm), lambda i: (i, 0))] * nh
    in_specs += [cols(p.shape[0]) for v in a for p in v] + pieces * (both * has_acc)
    sums = [jax.ShapeDtypeStruct((r, dm), F32) for r in sizes]
    wide = [jax.ShapeDtypeStruct((rows, f), BF)] * nh
    outs, out_specs = (wide + sums) * both, ([cols(rows)] * nh + pieces) * both
    if mode == "fwd":
        outs, out_specs = [jax.ShapeDtypeStruct((rows, f), F32)] * nh + outs, [cols(rows)] * nh + out_specs
    outs, out_specs = outs + [jax.ShapeDtypeStruct((rows, dm), BF)] * both, out_specs + [whole(rows)] * both
    res = pl.pallas_call(
        functools.partial(_pass_kernel, mode, nx, nh, len(a[0]) if a else 0, has_acc),
        grid=(f // TILE,), in_specs=in_specs, out_specs=out_specs, out_shape=outs,
        compiler_params=pltpu.CompilerParams(vmem_limit_bytes=60 << 20, dimension_semantics=("arbitrary",)),
        cost_estimate=pl.CostEstimate(flops=4 * both * rows * dm * f * nh, transcendentals=rows * f * nh,
                                      bytes_accessed=4 * nh * dm * f + 8 * rows * dm),
    )(*args)
    out = []
    for k in [nh] * (mode == "fwd") + [nh, nx] * both + [both]:
        out.append(list(res[:k]))
        res = res[k:]
    return out


def solution(mesh):
    rows = P(("data", "tp"), None)
    n = mesh.shape["tp"]
    up = [(i, (i + 2) % n) for i in range(n)]
    down = [(i, (i - 2) % n) for i in range(n)]
    over = [(i, (i + 4) % n) for i in range(n)]
    swap = [(i, i ^ 1) for i in range(n)]
    cat = jnp.concatenate

    def body(X, gamma, W1, W2, dY):
        last = [None]

        def step(f, *args):
            if last[0] is not None:
                args, _ = lax.optimization_barrier((args, last[0]))
            out = f(*args)
            last[0] = jax.tree.leaves(out)[0]
            return out

        def send(v, perm):
            if last[0] is not None:
                v, _ = lax.optimization_barrier((v, last[0]))
            return lax.ppermute(v, "tp", perm)

        h = X.shape[0] // 2
        W1p = send(W1, swap)
        g = step(lambda v: (v[:h], v[h:]), dY)
        g0u = send(g[0], up)
        g0d = send(g[1], down)
        xn = step(_norm, X, gamma)
        x0u = send(xn[0], up)
        x0d = send(xn[1], down)
        x1u = send(xn[1], up)
        x1d = send(xn[0], down)
        W2p = send(W2, swap)

        Hoa, Yo, dAoa, dXo, (Xo, _) = step(lambda x, g, w: _pass("both", [w], xs=x, gs=g), xn, g, (W1, W2))
        x2u = send(x0u, up)
        x2d = send(x0d, down)
        g1u = send(g[1], up)
        g1d = send(g[0], down)
        g2u = send(g0u, up)
        g2d = send(g0d, down)
        Gp0 = send(dY, swap)
        Xp0 = send(Xo, swap)

        ws = [(W1, W2), (W1p, W2p)]
        Ae, He, Ye, (Xe,) = step(lambda x, w: _pass("fwd", w, xs=x), (x1d, x0d, x0u, x1u), ws)
        Xp1 = send(Xe, swap)
        Hp1 = send(He[1], swap)
        Af, Hf, Yf, (Xf,) = step(lambda x, w: _pass("fwd", w, xs=x), (x2u, x2d), ws)
        yfu = send(Yf[0], up)
        yfd = send(Yf[1], down)
        ypu = send(Ye[1], up)
        ypd = send(Ye[2], down)
        Xp2 = send(Xf, swap)
        Hp2 = send(Hf[1], swap)

        dAr, dXr, (Gr,) = step(lambda g, w, a: _pass("bwd", w, gs=g, a=a),
                               (g1d, g0d, g0u, g1u, g2u, g2d), ws, list(zip(Ae, Af)))
        xfu = send(dXr[4], up)
        xfd = send(dXr[5], down)
        xpu = send(dXr[1], up)
        xpd = send(dXr[2], down)
        Dp1 = send(dAr[1], swap)
        Gp1 = send(Gr, swap)

        Hob, Yo, dAob, dXo, _ = step(lambda x, g, w, y, d: _pass("both", [w], xs=x, gs=g, y=y, d=d),
                                     xn, g, (W1p, W2p), Yo, dXo)
        Hp0 = send(Hob[0], swap)
        Dp0 = send(dAob[0], swap)

        dW1 = step(lambda a, b: _tn(cat(a), cat(b)), [Xo, Xe, Xf, Xp0, Xp1, Xp2], [dAoa[0], dAr[0], Dp0, Dp1])

        add2 = lambda a, b, u, d: (a + u, b + d)
        xqu, xqd = step(add2, dXr[0], dXr[3], xfu, xfd)
        xqu = send(xqu, up)
        xqd = send(xqd, down)
        yqu, yqd = step(add2, Ye[0], Ye[3], yfu, yfd)
        yqu = send(yqu, up)
        yqd = send(yqd, down)
        dW2 = step(lambda a, b: _tn(cat(a), cat(b)), [Hoa[0], He[0], Hf[0], Hp0, Hp1, Hp2], [dY, Gr, Gp0, Gp1])

        Yt = step(lambda yo, u, d: X.astype(F32) + (cat(yo) + cat([d, u])), Yo, ypu, ypd)

        def fin(dxo, xpu, xqu, xpd, xqd):
            dXn = cat(dxo) + cat([xqu, xpu]) + cat([xpd, xqd])
            xhatv, rstd = _ln(X.astype(F32))
            dgam = jnp.sum(dXn * xhatv, axis=0, keepdims=True)
            dxhat = dXn * gamma
            dx = rstd * (dxhat - jnp.mean(dxhat, axis=-1, keepdims=True) - xhatv * jnp.mean(dxhat * xhatv, axis=-1, keepdims=True))
            return (dY.astype(F32) + dx).astype(BF), dgam

        dX, dgam = step(fin, dXo, xpu, xqu, xpd, xqd)
        dgam = step(lambda a, b: a + b, dgam, send(dgam, swap))
        dgs = send(dgam, up), send(dgam, down), send(dgam, over)

        Y = step(lambda t, u, d: (t + cat([u, d])).astype(BF), Yt, yqu, yqd)
        dgam = dgam + dgs[0] + dgs[1] + dgs[2]
        return Y, dX, dW1, dW2, dgam[0]

    return jax.shard_map(body, mesh=mesh,
                         in_specs=(rows, P(None), P(None, "tp"), P("tp", None), rows),
                         out_specs=(rows, rows, P("data", "tp"), rows, P("data")),
                         check_vma=False)
```

```python
import functools

import jax
import jax.numpy as jnp
from jax import lax
from jax.experimental import pallas as pl
from jax.experimental.pallas import tpu as pltpu
from jax.sharding import PartitionSpec as P

EPS = 1e-6
BF = jnp.bfloat16
F32 = jnp.float32


def _gelu(a):
    return jax.nn.gelu(a, approximate=True)


def _ln(x):
    mu = jnp.mean(x, axis=-1, keepdims=True)
    xc = x - mu
    var = jnp.mean(xc * xc, axis=-1, keepdims=True)
    rstd = lax.rsqrt(var + EPS)
    return xc * rstd, rstd


def _tn(a, b):
    return lax.dot_general(a, b, (((0,), (0,)), ((), ())), preferred_element_type=F32)


TILE = 256
NCH = 512


def _nt(a, b):
    return lax.dot_general(a, b, (((1,), (1,)), ((), ())), preferred_element_type=F32)


def _ln_kernel(x_ref, gamma_ref, top_ref, bot_ref):
    h = top_ref.shape[0]
    gamma = gamma_ref[...]
    for out, r in ((top_ref, 0), (bot_ref, h)):
        out[...] = (_ln(x_ref[r:r + h, :].astype(F32))[0] * gamma).astype(BF)


def _norm(x, gamma):
    h = x.shape[0] // 2
    half = jax.ShapeDtypeStruct((h, x.shape[1]), BF)
    return pl.pallas_call(
        _ln_kernel, out_shape=(half, half), name="norm",
        compiler_params=pltpu.CompilerParams(vmem_limit_bytes=48 << 20),
        cost_estimate=pl.CostEstimate(flops=20 * x.size, bytes_accessed=4 * x.size, transcendentals=0),
    )(x, gamma.reshape(1, -1))


def _pass_kernel(mode, nx, nh, na, has_acc, *refs):
    refs = list(refs)

    def take(k):
        out, refs[:k] = refs[:k], []
        return out

    fwd, bwd = mode != "bwd", mode != "fwd"
    xs = take(nx) if fwd else []
    gs = take(nx) if bwd else []
    w1, w2 = take(nh), take(nh)
    a_in = [take(na) for _ in range(nh)] if not fwd else []
    y_in = take(nx) if fwd and has_acc else None
    d_in = take(nx) if bwd and has_acc else None
    a_out = take(nh) if mode == "fwd" else []
    h_out = take(nh) if fwd else []
    y_out = take(nx) if fwd else []
    da_out = take(nh) if bwd else []
    d_out = take(nx) if bwd else []
    xv = take(1)[0] if fwd else None
    gv = take(1)[0] if bwd else None

    @pl.when(pl.program_id(0) == 0)
    def _():
        for parts, v in ((xs, xv), (gs, gv)):
            r = 0
            for p in parts:
                v[r:r + p.shape[0], :] = p[...]
                r += p.shape[0]
        for outs, ins in ((y_out, y_in), (d_out, d_in)):
            for j, o in enumerate(outs):
                o[...] = ins[j][...] if ins else jnp.zeros_like(o)

    if fwd:
        a = [jnp.dot(xv[...], w1[k][...], preferred_element_type=F32) for k in range(nh)]
        h = [_gelu(v).astype(BF) for v in a]
        for k in range(nh):
            h_out[k][...] = h[k]
            if a_out:
                a_out[k][...] = a[k]
    else:
        a = [jnp.concatenate([p[...] for p in v]) for v in a_in]
    if bwd:
        dh = [_nt(gv[...], w2[k][...]) for k in range(nh)]
        da = [jax.vjp(_gelu, a[k])[1](dh[k])[0].astype(BF) for k in range(nh)]
        for k in range(nh):
            da_out[k][...] = da[k]

    def add(outs, n, v):
        r = 0
        for o in outs:
            m = o.shape[0]
            o[:, n:n + NCH] += v[r:r + m]
            r += m

    for n in range(0, w2[0].shape[1], NCH):
        if fwd:
            add(y_out, n, sum(jnp.dot(h[k], w2[k][:, n:n + NCH], preferred_element_type=F32) for k in range(nh)))
        if bwd:
            add(d_out, n, sum(_nt(da[k], w1[k][n:n + NCH, :]) for k in range(nh)))


def _pass(mode, ws, xs=(), gs=(), a=(), y=(), d=()):
    fwd, bwd = mode != "bwd", mode != "fwd"
    sizes = [p.shape[0] for p in (xs if fwd else gs)]
    nx, nh = len(sizes), len(ws)
    dm, f = ws[0][0].shape
    rows = sum(sizes)
    both = fwd + bwd
    once = pl.Buffered(buffer_count=1)

    def whole(r):
        return pl.BlockSpec((r, dm), lambda i: (0, 0), pipeline_mode=once)

    def cols(r):
        return pl.BlockSpec((r, TILE), lambda i: (0, i))

    pieces = [whole(r) for r in sizes]
    has_acc = bool(y or d)
    args = list(xs) * fwd + list(gs) * bwd + [w[0] for w in ws] + [w[1] for w in ws] + [p for v in a for p in v] + list(y) + list(d)
    in_specs = pieces * both + [cols(dm)] * nh + [pl.BlockSpec((TILE, dm), lambda i: (i, 0))] * nh
    in_specs += [cols(p.shape[0]) for v in a for p in v] + pieces * (both * has_acc)
    sums = [jax.ShapeDtypeStruct((r, dm), F32) for r in sizes]
    wide = [jax.ShapeDtypeStruct((rows, f), BF)] * nh
    outs, out_specs = (wide + sums) * both, ([cols(rows)] * nh + pieces) * both
    if mode == "fwd":
        outs, out_specs = [jax.ShapeDtypeStruct((rows, f), F32)] * nh + outs, [cols(rows)] * nh + out_specs
    outs, out_specs = outs + [jax.ShapeDtypeStruct((rows, dm), BF)] * both, out_specs + [whole(rows)] * both
    res = pl.pallas_call(
        functools.partial(_pass_kernel, mode, nx, nh, len(a[0]) if a else 0, has_acc),
        grid=(f // TILE,), in_specs=in_specs, out_specs=out_specs, out_shape=outs,
        compiler_params=pltpu.CompilerParams(vmem_limit_bytes=60 << 20, dimension_semantics=("arbitrary",)),
        cost_estimate=pl.CostEstimate(flops=4 * both * rows * dm * f * nh, transcendentals=rows * f * nh,
                                      bytes_accessed=4 * nh * dm * f + 8 * rows * dm),
    )(*args)
    out = []
    for k in [nh] * (mode == "fwd") + [nh, nx] * both + [both]:
        out.append(list(res[:k]))
        res = res[k:]
    return out


def _grad_kernel(k, chunk, *refs):
    a, b, out, bv, av, sems = refs[:k], refs[k:2 * k], refs[2 * k], refs[2 * k + 1], refs[2 * k + 2], refs[2 * k + 3]
    r, rows = 0, []
    for p in a:
        rows.append((r, p.shape[0]))
        r += p.shape[0]

    @pl.when(pl.program_id(0) == 0)
    def _():
        copies = [pltpu.make_async_copy(b[j], bv.at[pl.ds(r, m), :], sems.at[j]) for j, (r, m) in enumerate(rows)]
        for c in copies:
            c.start()
        for c in copies:
            c.wait()

    for j, (r, m) in enumerate(rows):
        av[r:r + m, :] = a[j][...]

    @pl.loop(0, out.shape[1] // chunk)
    def _(i):
        n = pl.multiple_of(i * chunk, chunk)
        out[:, pl.ds(n, chunk)] = _tn(av[...], bv[:, pl.ds(n, chunk)])


def _grad(a, b, tile, chunk):
    k, rows, m, n = len(a), sum(p.shape[0] for p in a), a[0].shape[1], b[0].shape[1]
    return pl.pallas_call(
        functools.partial(_grad_kernel, k, chunk), grid=(m // tile,),
        in_specs=[pl.BlockSpec((p.shape[0], tile), lambda i: (0, i)) for p in a] + [pl.BlockSpec(memory_space=pl.ANY)] * k,
        out_specs=pl.BlockSpec((tile, n), lambda i: (i, 0)), out_shape=jax.ShapeDtypeStruct((m, n), F32),
        scratch_shapes=[pltpu.VMEM((rows, n), BF), pltpu.VMEM((rows, tile), BF), pltpu.SemaphoreType.DMA((k,))],
        compiler_params=pltpu.CompilerParams(vmem_limit_bytes=60 << 20, dimension_semantics=("arbitrary",)),
        cost_estimate=pl.CostEstimate(flops=2 * rows * m * n, transcendentals=0, bytes_accessed=2 * rows * (m + n) + 4 * m * n),
    )(*a, *b)


def solution(mesh):
    rows = P(("data", "tp"), None)
    n = mesh.shape["tp"]
    up = [(i, (i + 2) % n) for i in range(n)]
    down = [(i, (i - 2) % n) for i in range(n)]
    over = [(i, (i + 4) % n) for i in range(n)]
    swap = [(i, i ^ 1) for i in range(n)]
    cat = jnp.concatenate

    def body(X, gamma, W1, W2, dY):
        last = [None]

        def step(f, *args):
            if last[0] is not None:
                args, _ = lax.optimization_barrier((args, last[0]))
            out = f(*args)
            last[0] = jax.tree.leaves(out)[0]
            return out

        def send(v, perm):
            if last[0] is not None:
                v, _ = lax.optimization_barrier((v, last[0]))
            return lax.ppermute(v, "tp", perm)

        h = X.shape[0] // 2
        W1p = send(W1, swap)
        g = step(lambda v: (v[:h], v[h:]), dY)
        g0u = send(g[0], up)
        g0d = send(g[1], down)
        xn = step(_norm, X, gamma)
        x0u = send(xn[0], up)
        x0d = send(xn[1], down)
        x1u = send(xn[1], up)
        x1d = send(xn[0], down)
        W2p = send(W2, swap)

        Hoa, Yo, dAoa, dXo, (Xo, _) = step(lambda x, g, w: _pass("both", [w], xs=x, gs=g), xn, g, (W1, W2))
        x2u = send(x0u, up)
        x2d = send(x0d, down)
        g1u = send(g[1], up)
        g1d = send(g[0], down)
        g2u = send(g0u, up)
        g2d = send(g0d, down)
        Hob, Yo, dAob, dXo, _ = step(lambda x, g, w, y, d: _pass("both", [w], xs=x, gs=g, y=y, d=d),
                                     xn, g, (W1p, W2p), Yo, dXo)
        Gp0 = send(dY, swap)
        Xp0 = send(Xo, swap)
        Hp0 = send(Hob[0], swap)
        Dp0 = send(dAob[0], swap)

        ws = [(W1, W2), (W1p, W2p)]
        Af, Hf, Yf, (Xf,) = step(lambda x, w: _pass("fwd", w, xs=x), (x2u, x2d), ws)
        yfu = send(Yf[0], up)
        yfd = send(Yf[1], down)
        Xp2 = send(Xf, swap)
        Hp2 = send(Hf[1], swap)
        Ae, He, Ye, (Xe,) = step(lambda x, w: _pass("fwd", w, xs=x), (x1d, x0d, x0u, x1u), ws)
        ypu = send(Ye[1], up)
        ypd = send(Ye[2], down)
        Xp1 = send(Xe, swap)
        Hp1 = send(He[1], swap)

        def back(gs, a):
            return step(lambda g, w, v: _pass("bwd", w, gs=g, a=v), gs, ws, [(v,) for v in a])

        dAf, dXf, (Gf,) = back((g2u, g2d), Af)
        xfu = send(dXf[0], up)
        xfd = send(dXf[1], down)
        Dp2 = send(dAf[1], swap)
        Gp2 = send(Gf, swap)
        dAe, dXe, (Ge,) = back((g1d, g0d, g0u, g1u), Ae)
        xpu = send(dXe[1], up)
        xpd = send(dXe[2], down)
        Dp1 = send(dAe[1], swap)
        Gp1 = send(Ge, swap)

        Yt = step(lambda yo, u, d: X.astype(F32) + (cat(yo) + cat([d, u])), Yo, ypu, ypd)

        add2 = lambda a, b, u, d: (a + u, b + d)
        xqu, xqd = step(add2, dXe[0], dXe[3], xfu, xfd)
        xqu = send(xqu, up)
        xqd = send(xqd, down)
        yqu, yqd = step(add2, Ye[0], Ye[3], yfu, yfd)
        yqu = send(yqu, up)
        yqd = send(yqd, down)
        dW1 = step(lambda a, b: _grad(a, b, 512, 896), [Xo, Xe, Xf, Xp0, Xp1, Xp2], [dAoa[0], dAe[0], dAf[0], Dp0, Dp1, Dp2])
        dW2 = step(lambda a, b: _grad(a, b, 256, 1024), [Hoa[0], He[0], Hf[0], Hp0, Hp1, Hp2], [dY, Ge, Gf, Gp0, Gp1, Gp2])

        def fin(dxo, xpu, xqu, xpd, xqd):
            dXn = cat(dxo) + cat([xqu, xpu]) + cat([xpd, xqd])
            xhatv, rstd = _ln(X.astype(F32))
            dgam = jnp.sum(dXn * xhatv, axis=0, keepdims=True)
            dxhat = dXn * gamma
            dx = rstd * (dxhat - jnp.mean(dxhat, axis=-1, keepdims=True) - xhatv * jnp.mean(dxhat * xhatv, axis=-1, keepdims=True))
            return (dY.astype(F32) + dx).astype(BF), dgam

        dX, dgam = step(fin, dXo, xpu, xqu, xpd, xqd)
        dgam = step(lambda a, b: a + b, dgam, send(dgam, swap))
        dgs = send(dgam, up), send(dgam, down), send(dgam, over)

        Y = step(lambda t, u, d: (t + cat([u, d])).astype(BF), Yt, yqu, yqd)
        dgam = dgam + dgs[0] + dgs[1] + dgs[2]
        return Y, dX, dW1, dW2, dgam[0]

    return jax.shard_map(body, mesh=mesh,
                         in_specs=(rows, P(None), P(None, "tp"), P("tp", None), rows),
                         out_specs=(rows, rows, P("data", "tp"), rows, P("data")),
                         check_vma=False)
```

```python
import functools

import jax
import jax.numpy as jnp
from jax import lax
from jax.experimental import pallas as pl
from jax.experimental.pallas import tpu as pltpu
from jax.sharding import PartitionSpec as P

EPS = 1e-6
BF = jnp.bfloat16
F32 = jnp.float32


def _gelu(a):
    return jax.nn.gelu(a, approximate=True)


def _ln(x):
    mu = jnp.mean(x, axis=-1, keepdims=True)
    xc = x - mu
    var = jnp.mean(xc * xc, axis=-1, keepdims=True)
    rstd = lax.rsqrt(var + EPS)
    return xc * rstd, rstd


def _tn(a, b):
    return lax.dot_general(a, b, (((0,), (0,)), ((), ())), preferred_element_type=F32)


TILE = 256
NCH = 512


def _nt(a, b):
    return lax.dot_general(a, b, (((1,), (1,)), ((), ())), preferred_element_type=F32)


def _ln_kernel(x_ref, gamma_ref, top_ref, bot_ref):
    h = top_ref.shape[0]
    gamma = gamma_ref[...]
    for out, r in ((top_ref, 0), (bot_ref, h)):
        out[...] = (_ln(x_ref[r:r + h, :].astype(F32))[0] * gamma).astype(BF)


STEP = 32


def _last_kernel(k, t_ref, u_ref, d_ref, *refs):
    i = pl.program_id(0)

    @pl.when(i < k)
    def _():
        refs[-1][...] = (t_ref[...] + u_ref[...]).astype(BF)

    @pl.when(i >= k)
    def _():
        refs[-1][...] = (t_ref[...] + d_ref[...]).astype(BF)


def _last(t, u, d, y=None):
    rows, dm = t.shape
    half, k = rows // 2 // STEP, u.shape[0] // STEP
    off = 0 if y is None else half - 1

    def block(f):
        return pl.BlockSpec((STEP, dm), lambda i: (f(i), 0))

    place = block(lambda i: off + jnp.where(i < k, i, i - k + half))
    return pl.pallas_call(
        functools.partial(_last_kernel, k), grid=(2 * k,), out_shape=jax.ShapeDtypeStruct((rows, dm), BF),
        in_specs=[place, block(lambda i: jnp.minimum(i, k - 1)), block(lambda i: jnp.maximum(i - k, 0))]
        + ([] if y is None else [pl.BlockSpec(memory_space=pl.ANY)]),
        out_specs=place, input_output_aliases={} if y is None else {3: 0},
        compiler_params=pltpu.CompilerParams(dimension_semantics=("arbitrary",)),
        cost_estimate=pl.CostEstimate(flops=4 * u.size, bytes_accessed=20 * u.size, transcendentals=0),
    )(t, u, d, *(() if y is None else (y,)))


def _norm(x, gamma):
    h = x.shape[0] // 2
    half = jax.ShapeDtypeStruct((h, x.shape[1]), BF)
    return pl.pallas_call(
        _ln_kernel, out_shape=(half, half), name="norm",
        compiler_params=pltpu.CompilerParams(vmem_limit_bytes=48 << 20),
        cost_estimate=pl.CostEstimate(flops=20 * x.size, bytes_accessed=4 * x.size, transcendentals=0),
    )(x, gamma.reshape(1, -1))


def _pass_kernel(mode, nx, nh, na, has_acc, *refs):
    refs = list(refs)

    def take(k):
        out, refs[:k] = refs[:k], []
        return out

    fwd, bwd = mode != "bwd", mode != "fwd"
    xs = take(nx) if fwd else []
    gs = take(nx) if bwd else []
    w1, w2 = take(nh), take(nh)
    a_in = [take(na) for _ in range(nh)] if not fwd else []
    y_in = take(nx) if fwd and has_acc else None
    d_in = take(nx) if bwd and has_acc else None
    a_out = take(nh) if mode == "fwd" else []
    h_out = take(nh) if fwd else []
    y_out = take(nx) if fwd else []
    da_out = take(nh) if bwd else []
    d_out = take(nx) if bwd else []
    xv = take(1)[0] if fwd else None
    gv = take(1)[0] if bwd else None

    @pl.when(pl.program_id(0) == 0)
    def _():
        for parts, v in ((xs, xv), (gs, gv)):
            r = 0
            for p in parts:
                v[r:r + p.shape[0], :] = p[...]
                r += p.shape[0]
        for outs, ins in ((y_out, y_in), (d_out, d_in)):
            for j, o in enumerate(outs):
                o[...] = ins[j][...] if ins else jnp.zeros_like(o)

    if fwd:
        a = [jnp.dot(xv[...], w1[k][...], preferred_element_type=F32) for k in range(nh)]
        h = [_gelu(v).astype(BF) for v in a]
        for k in range(nh):
            h_out[k][...] = h[k]
            if a_out:
                a_out[k][...] = a[k]
    else:
        a = [jnp.concatenate([p[...] for p in v]) for v in a_in]
    if bwd:
        dh = [_nt(gv[...], w2[k][...]) for k in range(nh)]
        da = [jax.vjp(_gelu, a[k])[1](dh[k])[0].astype(BF) for k in range(nh)]
        for k in range(nh):
            da_out[k][...] = da[k]

    def add(outs, n, v):
        r = 0
        for o in outs:
            m = o.shape[0]
            o[:, n:n + NCH] += v[r:r + m]
            r += m

    for n in range(0, w2[0].shape[1], NCH):
        if fwd:
            add(y_out, n, sum(jnp.dot(h[k], w2[k][:, n:n + NCH], preferred_element_type=F32) for k in range(nh)))
        if bwd:
            add(d_out, n, sum(_nt(da[k], w1[k][n:n + NCH, :]) for k in range(nh)))


def _pass(mode, ws, xs=(), gs=(), a=(), y=(), d=()):
    fwd, bwd = mode != "bwd", mode != "fwd"
    sizes = [p.shape[0] for p in (xs if fwd else gs)]
    nx, nh = len(sizes), len(ws)
    dm, f = ws[0][0].shape
    rows = sum(sizes)
    both = fwd + bwd
    once = pl.Buffered(buffer_count=1)

    def whole(r):
        return pl.BlockSpec((r, dm), lambda i: (0, 0), pipeline_mode=once)

    def cols(r):
        return pl.BlockSpec((r, TILE), lambda i: (0, i))

    pieces = [whole(r) for r in sizes]
    has_acc = bool(y or d)
    args = list(xs) * fwd + list(gs) * bwd + [w[0] for w in ws] + [w[1] for w in ws] + [p for v in a for p in v] + list(y) + list(d)
    in_specs = pieces * both + [cols(dm)] * nh + [pl.BlockSpec((TILE, dm), lambda i: (i, 0))] * nh
    in_specs += [cols(p.shape[0]) for v in a for p in v] + pieces * (both * has_acc)
    sums = [jax.ShapeDtypeStruct((r, dm), F32) for r in sizes]
    wide = [jax.ShapeDtypeStruct((rows, f), BF)] * nh
    outs, out_specs = (wide + sums) * both, ([cols(rows)] * nh + pieces) * both
    if mode == "fwd":
        outs, out_specs = [jax.ShapeDtypeStruct((rows, f), F32)] * nh + outs, [cols(rows)] * nh + out_specs
    outs, out_specs = outs + [jax.ShapeDtypeStruct((rows, dm), BF)] * both, out_specs + [whole(rows)] * both
    res = pl.pallas_call(
        functools.partial(_pass_kernel, mode, nx, nh, len(a[0]) if a else 0, has_acc),
        grid=(f // TILE,), in_specs=in_specs, out_specs=out_specs, out_shape=outs,
        compiler_params=pltpu.CompilerParams(vmem_limit_bytes=60 << 20, dimension_semantics=("arbitrary",)),
        cost_estimate=pl.CostEstimate(flops=4 * both * rows * dm * f * nh, transcendentals=rows * f * nh,
                                      bytes_accessed=4 * nh * dm * f + 8 * rows * dm),
    )(*args)
    out = []
    for k in [nh] * (mode == "fwd") + [nh, nx] * both + [both]:
        out.append(list(res[:k]))
        res = res[k:]
    return out


def _grad_kernel(k, chunk, *refs):
    a, b, out, bv, av, sems = refs[:k], refs[k:2 * k], refs[2 * k], refs[2 * k + 1], refs[2 * k + 2], refs[2 * k + 3]
    r, rows = 0, []
    for p in a:
        rows.append((r, p.shape[0]))
        r += p.shape[0]

    @pl.when(pl.program_id(0) == 0)
    def _():
        copies = [pltpu.make_async_copy(b[j], bv.at[pl.ds(r, m), :], sems.at[j]) for j, (r, m) in enumerate(rows)]
        for c in copies:
            c.start()
        for c in copies:
            c.wait()

    for j, (r, m) in enumerate(rows):
        av[r:r + m, :] = a[j][...]

    @pl.loop(0, out.shape[1] // chunk)
    def _(i):
        n = pl.multiple_of(i * chunk, chunk)
        out[:, pl.ds(n, chunk)] = _tn(av[...], bv[:, pl.ds(n, chunk)])


def _grad(a, b, tile, chunk):
    k, rows, m, n = len(a), sum(p.shape[0] for p in a), a[0].shape[1], b[0].shape[1]
    return pl.pallas_call(
        functools.partial(_grad_kernel, k, chunk), grid=(m // tile,),
        in_specs=[pl.BlockSpec((p.shape[0], tile), lambda i: (0, i)) for p in a] + [pl.BlockSpec(memory_space=pl.ANY)] * k,
        out_specs=pl.BlockSpec((tile, n), lambda i: (i, 0)), out_shape=jax.ShapeDtypeStruct((m, n), F32),
        scratch_shapes=[pltpu.VMEM((rows, n), BF), pltpu.VMEM((rows, tile), BF), pltpu.SemaphoreType.DMA((k,))],
        compiler_params=pltpu.CompilerParams(vmem_limit_bytes=60 << 20, dimension_semantics=("arbitrary",)),
        cost_estimate=pl.CostEstimate(flops=2 * rows * m * n, transcendentals=0, bytes_accessed=2 * rows * (m + n) + 4 * m * n),
    )(*a, *b)


def solution(mesh):
    rows = P(("data", "tp"), None)
    n = mesh.shape["tp"]
    up = [(i, (i + 2) % n) for i in range(n)]
    down = [(i, (i - 2) % n) for i in range(n)]
    over = [(i, (i + 4) % n) for i in range(n)]
    swap = [(i, i ^ 1) for i in range(n)]
    cat = jnp.concatenate

    def body(X, gamma, W1, W2, dY):
        last = [None]

        def step(f, *args):
            if last[0] is not None:
                args, _ = lax.optimization_barrier((args, last[0]))
            out = f(*args)
            last[0] = jax.tree.leaves(out)[0]
            return out

        def send(v, perm):
            if last[0] is not None:
                v, _ = lax.optimization_barrier((v, last[0]))
            return lax.ppermute(v, "tp", perm)

        h = X.shape[0] // 2
        W1p = send(W1, swap)
        g = step(lambda v: (v[:h], v[h:]), dY)
        g0u = send(g[0], up)
        g0d = send(g[1], down)
        xn = step(_norm, X, gamma)
        x0u = send(xn[0], up)
        x0d = send(xn[1], down)
        x1u = send(xn[1], up)
        x1d = send(xn[0], down)
        W2p = send(W2, swap)

        Hoa, Yo, dAoa, dXo, (Xo, _) = step(lambda x, g, w: _pass("both", [w], xs=x, gs=g), xn, g, (W1, W2))
        x2u = send(x0u, up)
        x2d = send(x0d, down)
        g1u = send(g[1], up)
        g1d = send(g[0], down)
        g2u = send(g0u, up)
        g2d = send(g0d, down)
        Hob, Yo, dAob, dXo, _ = step(lambda x, g, w, y, d: _pass("both", [w], xs=x, gs=g, y=y, d=d),
                                     xn, g, (W1p, W2p), Yo, dXo)
        Gp0 = send(dY, swap)
        Xp0 = send(Xo, swap)
        Hp0 = send(Hob[0], swap)
        Dp0 = send(dAob[0], swap)

        ws = [(W1, W2), (W1p, W2p)]
        Af, Hf, Yf, (Xf,) = step(lambda x, w: _pass("fwd", w, xs=x), (x2u, x2d), ws)
        yfu = send(Yf[0], up)
        yfd = send(Yf[1], down)
        Xp2 = send(Xf, swap)
        Hp2 = send(Hf[1], swap)
        Ae, He, Ye, (Xe,) = step(lambda x, w: _pass("fwd", w, xs=x), (x1d, x0d, x0u, x1u), ws)
        ypu = send(Ye[1], up)
        ypd = send(Ye[2], down)
        Xp1 = send(Xe, swap)
        Hp1 = send(He[1], swap)

        def back(gs, a):
            return step(lambda g, w, v: _pass("bwd", w, gs=g, a=v), gs, ws, [(v,) for v in a])

        dAf, dXf, (Gf,) = back((g2u, g2d), Af)
        xfu = send(dXf[0], up)
        xfd = send(dXf[1], down)
        Dp2 = send(dAf[1], swap)
        Gp2 = send(Gf, swap)
        dAe, dXe, (Ge,) = back((g1d, g0d, g0u, g1u), Ae)
        xpu = send(dXe[1], up)
        xpd = send(dXe[2], down)
        Dp1 = send(dAe[1], swap)
        Gp1 = send(Ge, swap)

        Yt = step(lambda yo, u, d: X.astype(F32) + (cat(yo) + cat([d, u])), Yo, ypu, ypd)

        add2 = lambda a, b, u, d: (a + u, b + d)
        m = h - STEP
        yq = step(lambda a, b, u, d: (a[:m] + u[:m], b[:m] + d[:m], a[m:] + u[m:], b[m:] + d[m:]), Ye[0], Ye[3], yfu, yfd)
        xqu, xqd = step(add2, dXe[0], dXe[3], xfu, xfd)
        xqu = send(xqu, up)
        xqd = send(xqd, down)
        yqu = send(yq[0], up)
        yqd = send(yq[1], down)
        yru = send(yq[2], up)
        yrd = send(yq[3], down)

        dW1 = step(lambda a, b: _grad(a, b, 512, 896), [Xo, Xe, Xf, Xp0, Xp1, Xp2], [dAoa[0], dAe[0], dAf[0], Dp0, Dp1, Dp2])
        dW2 = step(lambda a, b: _grad(a, b, 256, 1024), [Hoa[0], He[0], Hf[0], Hp0, Hp1, Hp2], [dY, Ge, Gf, Gp0, Gp1, Gp2])

        def fin(dxo, xpu, xqu, xpd, xqd):
            dXn = cat(dxo) + cat([xqu, xpu]) + cat([xpd, xqd])
            xhatv, rstd = _ln(X.astype(F32))
            dgam = jnp.sum(dXn * xhatv, axis=0, keepdims=True)
            dxhat = dXn * gamma
            dx = rstd * (dxhat - jnp.mean(dxhat, axis=-1, keepdims=True) - xhatv * jnp.mean(dxhat * xhatv, axis=-1, keepdims=True))
            return (dY.astype(F32) + dx).astype(BF), dgam

        dX, dgam = step(fin, dXo, xpu, xqu, xpd, xqd)
        dgam = step(lambda a, b: a + b, dgam, send(dgam, swap))
        dgs = send(dgam, up), send(dgam, down), send(dgam, over)

        Y = step(lambda *v: _last(*v), Yt, yqu, yqd)
        Y = step(lambda *v: _last(*v), Yt, yru, yrd, Y)
        dgam = dgam + dgs[0] + dgs[1] + dgs[2]
        return Y, dX, dW1, dW2, dgam[0]

    return jax.shard_map(body, mesh=mesh,
                         in_specs=(rows, P(None), P(None, "tp"), P("tp", None), rows),
                         out_specs=(rows, rows, P("data", "tp"), rows, P("data")),
                         check_vma=False)
```
